32 devices in a mesh: seq: 16 (over z, x, core), res: 2 (over y).
Axes of the slice: x: 2, y: 2, z: 4, core: 2. Of those that a mesh axis runs over, the one named last changes fastest.
Arguments:
- alignment_rows: bfloat16 [1024, 16, 64], P('seq', 'res'), may hold values from -6 to 6
- pair_features: bfloat16 [16, 16, 128], P('res', 'seq'), may hold values from -6 to 6
- sequence_block_count: int32 [16], P('seq'), may hold values from 16 to 64
- cluster_member_count: int32 [1024], P('seq'), may hold values from 1 to 16
- residue_present_mask: int32 [16], replicated, may hold values 0 or 1
- attention_in_weight: bfloat16 [64, 256], replicated, may hold values from -0.75 to 0.75
- attention_out_weight: bfloat16 [64, 64], replicated, may hold values from -4 to 4
- pair_bias_weight: float32 [128, 8], replicated, may hold values from -48 to 48
- outer_factor_weight: bfloat16 [64, 64], replicated, may hold values from -0.75 to 0.75
- outer_output_weight: float32 [1024, 128], replicated, may hold values from -4 to 4
- outer_product_bias: float32 [128], replicated, may hold values from -3 to 3
Outputs:
- row_attention_update: bfloat16 [1024, 16, 64], P('seq', 'res')
- pair_update: bfloat16 [16, 16, 128], P('seq', 'res')
The draws below stay inside these ranges and needn't reach their ends.
All inputs are finite; a program needn't handle non-finite values.
Results may differ from the reference program's by a relative error of at most 0.0081.
Values may be sent and summed in bfloat16 or wider, within the bound.
A program may use at most 64 MiB of HBM per device.

```python
import math
import jax
import jax.numpy as jnp
from jax import lax

CHANNEL_COUNT = 64
CP = 128
CO = 32
HEADS = 8
HEAD_DIM = 8
SLOT_DEV = 64
RES_DEV = 8
SLOT_TOTAL = 1024
RESIDUE_TOTAL = 16
N_SEQ = 16
N_RES = 2


def draw_pair_bias_weight(key, part):
    values = jax.random.normal(key, (CP, HEADS), jnp.float32) * (2.0 / math.sqrt(CP))
    return jnp.clip(values, -48.0, 48.0)


def plant(values, key, low, top_value):
    index_at = [jax.random.randint(jax.random.fold_in(key, axis), (), 0, length) for axis, length in enumerate(values.shape)]
    widest = values.shape.index(max(values.shape))
    neighbour = index_at[:widest] + [(index_at[widest] + 1) % values.shape[widest]] + index_at[widest + 1:]
    return values.at[tuple(index_at)].set(low).at[tuple(neighbour)].set(top_value)


def level_of(key, shape, split, low, high):
    level = 1.0
    for position, blocks in split:
        steps = jax.random.uniform(jax.random.fold_in(jax.random.fold_in(key, 6), position), (blocks,), jnp.float32, low / len(split), high / len(split))
        level = level * jnp.repeat(jnp.exp(steps), shape[position] // blocks).reshape((-1,) + (1,) * (len(shape) - 1 - position))
    return level


def centred(rng, dims, scale, reach, split=(), kind=jnp.bfloat16):
    drawn = jax.random.normal(rng, dims, jnp.float32) * scale
    if len(split) > 0:
        drawn = level_of(rng, dims, split, -0.22, 0.18) * drawn
    return jnp.clip(drawn, min=-reach, max=reach).astype(kind)


def setup_inputs(seed: int = 0) -> dict:
    arg_keys = jax.random.split(jax.random.key(seed), 12)
    return {
        "alignment_rows": centred(arg_keys[0], (SLOT_TOTAL, RESIDUE_TOTAL, CHANNEL_COUNT), 1.0, 6.0, ((0, 16), (1, 2))),
        "pair_features": centred(arg_keys[1], (RESIDUE_TOTAL, RESIDUE_TOTAL, CP), 1.0, 6.0, ((0, 2), (1, 16))),
        "sequence_block_count": plant(jax.random.randint(arg_keys[2], (N_SEQ,), SLOT_DEV // 4, SLOT_DEV + 1), jax.random.fold_in(arg_keys[2], 1), SLOT_DEV // 4, SLOT_DEV).astype(jnp.int32),
        "cluster_member_count": plant(jax.random.randint(arg_keys[3], (SLOT_TOTAL,), 1, 17), jax.random.fold_in(arg_keys[3], 1), 1, 16).astype(jnp.int32),
        "residue_present_mask": plant((jax.random.randint(arg_keys[4], (RESIDUE_TOTAL,), 0, 8) < 7).astype(jnp.int32), jax.random.fold_in(arg_keys[4], 1), 0, 1),
        "attention_in_weight": centred(arg_keys[5], (CHANNEL_COUNT, 4 * CHANNEL_COUNT), CHANNEL_COUNT ** -0.5, 0.75),
        "attention_out_weight": centred(arg_keys[6], (CHANNEL_COUNT, CHANNEL_COUNT), 1.0, 4.0),
        "pair_bias_weight": draw_pair_bias_weight(jax.random.fold_in(arg_keys[11], 71), 0),
        "outer_factor_weight": centred(arg_keys[8], (CHANNEL_COUNT, 2 * CO), CHANNEL_COUNT ** -0.5, 0.75),
        "outer_output_weight": centred(arg_keys[9], (CO * CO, CP), 1.0, 4.0, (), jnp.float32),
        "outer_product_bias": centred(arg_keys[10], (CP,), 0.5, 3.0, (), jnp.float32),
    }


def apply_layer_norm(values):
    centre = lax.optimization_barrier(jnp.mean(values, axis=-1, keepdims=True))
    spread = lax.optimization_barrier(jnp.mean(jnp.square(values - centre), axis=-1, keepdims=True))
    return (values - centre) * lax.rsqrt(spread + 1e-05)

def attend_block(pieces, full_bias):
    query_rows, key_value_pairs, gate_activation = pieces
    slot_count, n_query, channel_width = query_rows.shape
    head_count = full_bias.shape[0]
    head_dim = channel_width // head_count
    n_keys = key_value_pairs.shape[1]
    query_heads = query_rows.astype(jnp.float32).reshape(slot_count, n_query, head_count, head_dim)
    key_heads = key_value_pairs[..., :channel_width].astype(jnp.float32).reshape(slot_count, n_keys, head_count, head_dim)
    value_heads = key_value_pairs[..., channel_width:].astype(jnp.float32).reshape(slot_count, n_keys, head_count, head_dim)
    scores = jnp.einsum('bihd,bjhd->bhij', query_heads, key_heads, precision=lax.Precision.HIGHEST) + full_bias[None]
    row_max = lax.optimization_barrier(jnp.max(scores, axis=-1, keepdims=True))
    expo = jnp.exp(scores - row_max)
    probs = (expo / lax.optimization_barrier(jnp.sum(expo, axis=-1, keepdims=True))).astype(jnp.bfloat16)
    context = jnp.einsum('bhij,bjhd->bihd', probs.astype(jnp.float32), value_heads, precision=lax.Precision.HIGHEST)
    return (gate_activation * context.reshape(slot_count, n_query, channel_width)).astype(jnp.bfloat16)

def reference(alignment_rows, pair_features, sequence_block_count, cluster_member_count, residue_present_mask, attention_in_weight, attention_out_weight, pair_bias_weight, outer_factor_weight, outer_output_weight, outer_product_bias):
    total_count = SLOT_DEV * N_SEQ
    block_length = RES_DEV * N_RES
    slot_ids = jnp.arange(total_count, dtype=jnp.int32)
    usable = (slot_ids % SLOT_DEV < sequence_block_count[slot_ids // SLOT_DEV]).astype(jnp.float32)
    seq_weight = cluster_member_count.astype(jnp.float32) * usable
    weight_sum = jnp.sum(seq_weight)
    key_mask = jnp.where(residue_present_mask == 1, 0.0, -1000000.0).astype(jnp.float32)
    pair_norm = apply_layer_norm(pair_features.astype(jnp.float32))
    pair_bias = jnp.einsum('ijp,ph->hij', pair_norm, pair_bias_weight, precision=lax.Precision.HIGHEST) + key_mask[None, None, :]
    normed_alignment = apply_layer_norm(alignment_rows.astype(jnp.float32)).astype(jnp.bfloat16)
    projected_rows = jnp.dot(normed_alignment.reshape(-1, CHANNEL_COUNT), attention_in_weight, preferred_element_type=jnp.float32).reshape(total_count, block_length, 4 * CHANNEL_COUNT)
    query_rows = (projected_rows[..., :CHANNEL_COUNT] * (1.0 / math.sqrt(HEAD_DIM))).astype(jnp.bfloat16)
    key_value_pairs = projected_rows[..., CHANNEL_COUNT:3 * CHANNEL_COUNT].astype(jnp.bfloat16)
    gate_activation = jax.nn.sigmoid(projected_rows[..., 3 * CHANNEL_COUNT:])
    gated = lax.map(lambda pieces: attend_block(pieces, pair_bias), (query_rows.reshape(N_SEQ, SLOT_DEV, block_length, CHANNEL_COUNT), key_value_pairs.reshape(N_SEQ, SLOT_DEV, block_length, 2 * CHANNEL_COUNT), gate_activation.reshape(N_SEQ, SLOT_DEV, block_length, CHANNEL_COUNT)))
    update = jnp.dot(gated.reshape(-1, CHANNEL_COUNT), attention_out_weight, preferred_element_type=jnp.float32).astype(jnp.bfloat16)
    row_attention_update = update.reshape(total_count, block_length, CHANNEL_COUNT) * usable.astype(jnp.bfloat16)[:, None, None]
    updated_alignment = alignment_rows.astype(jnp.float32) + row_attention_update.astype(jnp.float32)
    outer_input_norm = apply_layer_norm(updated_alignment).astype(jnp.bfloat16)
    factors = jnp.dot(outer_input_norm.reshape(-1, CHANNEL_COUNT), outer_factor_weight, preferred_element_type=jnp.float32).reshape(total_count, block_length, 2 * CO)
    res_keep = residue_present_mask.astype(jnp.float32)[None, :, None]
    left_proj = (factors[..., :CO] * res_keep).astype(jnp.bfloat16)
    right_proj = (factors[..., CO:] * res_keep * seq_weight[:, None, None]).astype(jnp.bfloat16)
    outer = lax.dot_general(left_proj.reshape(total_count, block_length * CO).astype(jnp.float32), right_proj.reshape(total_count, block_length * CO).astype(jnp.float32), (((0,), (0,)), ((), ())), precision=lax.Precision.HIGHEST)
    outer = outer.reshape(block_length, CO, block_length, CO)
    projected = jnp.einsum('icjd,cdp->ijp', outer, outer_output_weight.reshape(CO, CO, CP), precision=lax.Precision.HIGHEST)
    pair_update = (projected / weight_sum + outer_product_bias).astype(jnp.bfloat16)
    return (row_attention_update, pair_update)
```

```python
import functools
import math

import jax
import jax.numpy as jnp
from jax import lax
from jax.experimental import pallas as pl
from jax.experimental.pallas import tpu as pltpu
from jax.sharding import PartitionSpec as P

MESH = pl.DeviceIdType.MESH
F32 = jnp.float32
BF16 = jnp.bfloat16
LANES = 128


def dot(a, b, ca, cb, precision=None):
    return lax.dot_general(
        a, b, (((ca,), (cb,)), ((), ())), precision=precision, preferred_element_type=F32
    )


def norm_over(values, axis):
    centre = jnp.mean(values, axis=axis, keepdims=True)
    shifted = values - centre
    spread = jnp.mean(shifted * shifted, axis=axis, keepdims=True)
    return shifted * lax.rsqrt(spread + 1e-05)


def iota(shape, axis):
    return lax.broadcasted_iota(jnp.int32, shape, axis)


def ones_where(mask):
    return jnp.where(mask, 1.0, 0.0).astype(BF16)


def each(start, stop, body):
    if stop - start <= 16:
        for k in range(start, stop):
            body(k)
    else:
        pl.loop(start, stop)(body)


def kernel(
    n_seq,
    n_res,
    slots,
    rl,
    heads,
    factor,
    count_hbm,
    mask_hbm,
    x_hbm,
    pair_hbm,
    members_hbm,
    w_in_hbm,
    w_out_hbm,
    w_bias_hbm,
    w_fac_hbm,
    w_proj_hbm,
    bias_hbm,
    update_ref,
    pair_out_ref,
    count_ref,
    mask_ref,
    x_ref,
    pair_ref,
    members_ref,
    w_in_ref,
    w_out_ref,
    w_bias_ref,
    w_fac_ref,
    w_raw,
    bias_ref,
    rows32,
    x_t,
    xn_buf,
    xn_recv,
    tile_buf,
    tile_recv,
    pick_s,
    w_in_t,
    w_out_t,
    w_out_p,
    w_fac_t,
    kv_s,
    roll_s,
    gate_s,
    score_s,
    gated_s,
    left_buf,
    left_recv,
    right_s,
    outer_s,
    w_perm,
    part_buf,
    part_recv,
    in_sem,
    xn_send_sem,
    xn_recv_sem,
    tile_send_sem,
    tile_recv_sem,
    left_send_sem,
    left_recv_sem,
    part_send_sem,
    part_recv_sem,
):
    me_s = lax.axis_index("seq")
    me_r = lax.axis_index("res")
    width = x_ref.shape[2]
    hd = width // heads
    tiles = rl // 2
    row_block = rl * n_res // n_seq

    def seq_peer(k):
        return lax.rem(me_s + k, n_seq)

    def res_peer(k):
        return lax.rem(me_r + k, n_res)

    def res_of(block):
        return lax.rem(me_r + n_res - block, n_res)

    barrier = pltpu.get_barrier_semaphore()

    def greet(k):
        pl.semaphore_signal(barrier, inc=1, device_id=(seq_peer(k), me_r), device_id_type=MESH)

    each(1, n_seq, greet)
    for k in range(1, n_res):
        pl.semaphore_signal(barrier, inc=1, device_id=(me_s, res_peer(k)), device_id_type=MESH)

    loads = {}
    for at, (name, src, dst) in enumerate(
        [
            ("pair", pair_hbm, pair_ref),
            ("w_bias", w_bias_hbm, w_bias_ref),
            ("count", count_hbm, count_ref),
            ("members", members_hbm, members_ref),
            ("x", x_hbm, x_ref),
            ("w_in", w_in_hbm, w_in_ref),
            ("mask", mask_hbm, mask_ref),
            ("w_out", w_out_hbm, w_out_ref),
            ("w_fac", w_fac_hbm, w_fac_ref),
            ("w_proj", w_proj_hbm, w_raw),
            ("bias", bias_hbm, bias_ref),
        ]
    ):
        loads[name] = pltpu.make_async_copy(src, dst, in_sem.at[at])
        loads[name].start()

    def loaded(*names):
        for name in names:
            loads[name].wait()

    lane = iota((1, LANES), 1)
    low = lane < slots
    of_head = iota((heads, LANES), 1) // rl == iota((heads, LANES), 0)

    loaded("pair", "w_bias", "count", "members")
    count = count_ref[0]
    usable = (lax.rem(lane, slots) < count).astype(F32)
    members = members_ref[...].astype(F32)
    members = jnp.concatenate([members, members], axis=1)
    seq_weight = members * usable
    own_weight = jnp.sum(jnp.where(low, seq_weight, 0.0), axis=1, keepdims=True)

    pair_norm = norm_over(pair_ref[...].astype(F32), 1)
    bias_t = dot(
        w_bias_ref[...],
        jnp.concatenate([pair_norm] * (LANES // rl), axis=0),
        1,
        1,
        lax.Precision.HIGHEST,
    )
    packed = jnp.sum(jnp.where(of_head, bias_t, 0.0), axis=0, keepdims=True)
    packed = jnp.where(lane == LANES - 1, own_weight, packed)
    tile_buf[...] = packed
    tile_recv[me_s] = packed

    loaded("x")
    rows32[:, :width] = x_ref[...].astype(F32).reshape(slots * rl, width)
    eye = ones_where(iota((width, width), 0) == iota((width, width), 1))
    for t in range(tiles):
        pair_rows = jnp.concatenate(
            [rows32[pl.ds(2 * t + e, slots, stride=rl), :][:, :width] for e in range(2)], axis=0
        ).astype(BF16)
        turned = dot(eye, pair_rows, 1, 1)
        x_t[t] = turned
        xn_buf[t] = norm_over(turned, 0).astype(BF16)

    pl.semaphore_wait(barrier, n_seq - 1 + n_res - 1)

    def tile_copy(k):
        return pltpu.make_async_remote_copy(
            src_ref=tile_buf,
            dst_ref=tile_recv.at[me_s],
            send_sem=tile_send_sem.at[k - 1],
            recv_sem=tile_recv_sem.at[k - 1],
            device_id=(seq_peer(k), me_r),
            device_id_type=MESH,
        )

    each(1, n_seq, lambda k: tile_copy(k).start())

    xn_copies = [
        pltpu.make_async_remote_copy(
            src_ref=xn_buf,
            dst_ref=xn_recv.at[k - 1],
            send_sem=xn_send_sem.at[k - 1],
            recv_sem=xn_recv_sem.at[k - 1],
            device_id=(me_s, res_peer(k)),
            device_id_type=MESH,
        )
        for k in range(1, n_res)
    ]
    for copy in xn_copies:
        copy.start()

    loaded("w_in", "mask", "w_out", "w_fac", "w_proj", "bias")
    groups_in = w_in_ref.shape[1]
    to_row, from_col = iota((groups_in, groups_in), 0), iota((groups_in, groups_in), 1)
    order = (
        to_row // width * width
        + lax.rem(to_row, heads) * hd
        + lax.rem(to_row, width) // heads
    )
    perm = ones_where(order == from_col)
    w_in_t[...] = dot(perm, w_in_ref[...], 1, 1).astype(BF16)
    perm_out = perm[:width, :width]
    w_out_t[...] = dot(w_out_ref[...], perm_out, 0, 1).astype(BF16)
    w_out_p[...] = dot(perm_out, w_out_ref[...], 1, 0).astype(BF16)
    w_fac_t[...] = dot(w_fac_ref[...], eye, 0, 0).astype(BF16)

    row_k, col_l = iota((2 * LANES, LANES), 0), iota((2 * LANES, LANES), 1)
    half = (col_l >= slots).astype(jnp.int32)
    for t in range(tiles):
        for turn in range(2):
            hit = (lax.rem(row_k, rl) == 2 * t + half) & (
                row_k // LANES == (half if turn == 0 else 1 - half)
            )
            pick_s[t, :, turn * LANES : (turn + 1) * LANES] = ones_where(hit)

    scale = 1.0 / math.sqrt(hd)

    def put_kv(block, t, kv):
        kv = kv.astype(BF16).astype(F32)
        kv_s[block, t] = kv
        roll_s[block, t] = pltpu.roll(kv, slots, 1)

    queries = []
    for t in range(tiles):
        proj = dot(w_in_t[...], xn_buf[t], 1, 0)
        queries.append((proj[:width] * scale).astype(BF16).astype(F32))
        put_kv(0, t, proj[width : 3 * width])
        gate_s[t] = jax.nn.sigmoid(proj[3 * width :])

    for d in range(factor):
        w_perm[d * factor : (d + 1) * factor] = w_raw[pl.ds(d, factor, stride=factor), :].astype(BF16)

    combos = [(turn, block, u) for turn in range(2) for block in range(n_res) for u in range(tiles)]

    def score(block):
        for at, (turn, of, u) in enumerate(combos):
            if of != block:
                continue
            source = (roll_s if turn else kv_s).at[block, u]
            for t in range(tiles):
                total = None
                for d in range(hd):
                    term = queries[t][d * heads : (d + 1) * heads] * source[d * heads : (d + 1) * heads]
                    total = term if total is None else total + term
                score_s[t, at] = total

    score(0)
    for block in range(1, n_res):
        xn_copies[block - 1].wait()
        for t in range(tiles):
            put_kv(block, t, dot(w_in_t[width : 3 * width], xn_recv[block - 1, t], 1, 0))
        score(block)

    each(1, n_seq, lambda k: tile_copy(k).wait())

    weight_sum = jnp.sum(tile_recv[...], axis=0)[:, LANES - 1 : LANES]
    keyed = []
    for block in range(n_res):
        for u in range(tiles):
            sides = []
            for e in range(2):
                j = res_of(block) * rl + 2 * u + e
                key_mask = jnp.where(mask_ref[j] == 1, 0.0, -1000000.0).astype(F32)
                sides.append(jnp.where(of_head, tile_recv[j] + key_mask, 0.0))
            keyed.append(jnp.concatenate(sides, axis=1))
    keyed = jnp.concatenate(keyed, axis=0)
    pieces = []
    rest = keyed
    for _ in range(3):
        piece = rest.astype(BF16)
        pieces.append(piece)
        rest = rest - piece.astype(F32)
    pieces = jnp.concatenate(pieces, axis=0)
    n_rows = keyed.shape[0]

    left_copies = []
    for k in range(1, n_res):
        left_copies.append(
            [
                pltpu.make_async_remote_copy(
                    src_ref=left_buf.at[t],
                    dst_ref=left_recv.at[k - 1, t],
                    send_sem=left_send_sem.at[k - 1, t],
                    recv_sem=left_recv_sem.at[k - 1, t],
                    device_id=(me_s, res_peer(k)),
                    device_id_type=MESH,
                )
                for t in range(tiles)
            ]
        )

    rights = []
    for t in range(tiles):
        spread = dot(pieces, pick_s[t], 1, 0)
        spread = (spread[:n_rows] + spread[n_rows : 2 * n_rows]) + spread[2 * n_rows :]
        scores = []
        for at, (turn, block, u) in enumerate(combos):
            row = (block * tiles + u) * heads
            scores.append(
                score_s[t, at] + spread[row : row + heads, turn * LANES : (turn + 1) * LANES]
            )
        top = functools.reduce(jnp.maximum, scores)
        context = [None] * hd
        mass = None
        for at, (turn, block, u) in enumerate(combos):
            source = (roll_s if turn else kv_s).at[block, u]
            expo = jnp.exp(scores[at] - top)
            mass = expo if mass is None else mass + expo
            for d in range(hd):
                term = expo * source[width + d * heads : width + (d + 1) * heads]
                context[d] = term if context[d] is None else context[d] + term
        norm = 1.0 / mass
        context = jnp.concatenate([c * norm for c in context], axis=0)
        gated = (gate_s[t] * context).astype(BF16)
        gated_s[t] = gated
        update = dot(w_out_t[...], gated, 1, 0).astype(BF16).astype(F32) * usable
        outer_norm = norm_over(x_t[t] + update, 0).astype(BF16)
        factors = dot(w_fac_t[...], outer_norm, 1, 0)
        keeps = [(mask_ref[me_r * rl + 2 * t + e]).astype(F32) for e in range(2)]
        keep = jnp.where(low, keeps[0], keeps[1])
        left_buf[t] = (factors[:factor] * keep).astype(BF16)
        for copies in left_copies:
            copies[t].start()
        rights.append(factors[factor:] * keep * seq_weight)

    for t in range(tiles):
        right = rights[t]
        turned = pltpu.roll(right, slots, 1)
        zero = jnp.zeros_like(right)
        right_s[0, pl.ds(2 * t, factor, stride=rl), :] = jnp.where(low, right, zero)
        right_s[0, pl.ds(2 * t + 1, factor, stride=rl), :] = jnp.where(low, turned, zero)
        right_s[1, pl.ds(2 * t, factor, stride=rl), :] = jnp.where(low, zero, turned)
        right_s[1, pl.ds(2 * t + 1, factor, stride=rl), :] = jnp.where(low, zero, right)

    right_all = right_s[...].reshape(2 * factor * rl, LANES).astype(BF16)
    groups = LANES // factor
    even = lax.rem(lane // factor, 2) == 0

    def project(block, left):
        products = dot(right_all, left.reshape(tiles * factor, LANES), 1, 1)
        for half in range(2):
            for g in range(factor // groups):
                base = (half * factor + g * groups) * rl
                a = [products[base + k * rl : base + (k + 1) * rl] for k in range(groups)]
                p0 = jnp.where(low, a[0], pltpu.roll(a[2], 64, 1))
                p2 = jnp.where(low, pltpu.roll(a[0], 64, 1), a[2])
                p1 = jnp.where(low, a[1], pltpu.roll(a[3], 64, 1))
                p3 = jnp.where(low, pltpu.roll(a[1], 64, 1), a[3])
                out = [
                    jnp.where(even, p0, pltpu.roll(p1, 32, 1)),
                    jnp.where(even, pltpu.roll(p0, 96, 1), p1),
                    jnp.where(even, p2, pltpu.roll(p3, 32, 1)),
                    jnp.where(even, pltpu.roll(p2, 96, 1), p3),
                ]
                for ip in range(groups):
                    i = 2 * ip + half
                    outer_s[i * rl : (i + 1) * rl, g * LANES : (g + 1) * LANES] = out[ip]
        part = dot(outer_s[...].astype(BF16), w_perm[...], 1, 0)
        part_buf[pl.ds(res_of(block) * rl, rl)] = part.reshape(rl, rl, part.shape[1]).astype(BF16)

    def part_copy(owner, k):
        return pltpu.make_async_remote_copy(
            src_ref=part_buf.at[pl.ds(owner * row_block, row_block)],
            dst_ref=part_recv.at[k - 1],
            send_sem=part_send_sem.at[k - 1],
            recv_sem=part_recv_sem.at[k - 1],
            device_id=(owner, me_r),
            device_id_type=MESH,
        )

    def send_parts(block):
        for m in range(rl // row_block):
            owner = res_of(block) * (rl // row_block) + m
            offset = lax.rem(owner + n_seq - me_s, n_seq)

            @pl.when(offset > 0)
            def _():
                part_copy(owner, offset).start()

    project(0, left_buf[...])
    send_parts(0)
    for block in range(1, n_res):
        for t in range(tiles):
            left_copies[block - 1][t].wait()
        project(block, left_recv[block - 1])
        send_parts(block)

    row_usable = (iota((slots, 1), 0) < count).astype(F32)
    w_out_wide = jnp.concatenate([w_out_p[...], w_out_p[...]], axis=1)
    for t in range(tiles):
        plain = dot(gated_s[t], w_out_wide, 0, 0).astype(BF16).astype(F32)
        for e in range(2):
            rows32[pl.ds(2 * t + e, slots, stride=rl), :] = (
                plain[e * slots : (e + 1) * slots] * row_usable
            )
    update_ref[...] = rows32[:, :width].reshape(slots, rl, width).astype(BF16)

    each(1, n_seq, lambda k: part_copy(seq_peer(k), k).wait())

    own = part_buf[pl.ds(me_s * row_block, row_block)].astype(F32)
    total = own + jnp.sum(part_recv[...].astype(F32), axis=0)
    pair_out_ref[...] = (total / weight_sum[None] + bias_ref[...][None]).astype(BF16)


def finish(update_ref, pair_ref, update_hbm, pair_hbm, sem):
    copies = [
        pltpu.make_async_copy(update_ref, update_hbm, sem.at[0]),
        pltpu.make_async_copy(pair_ref, pair_hbm, sem.at[1]),
    ]
    for copy in copies:
        copy.start()
    for copy in copies:
        copy.wait()


def solution(mesh):
    n_seq = mesh.shape["seq"]
    n_res = mesh.shape["res"]

    def local(
        alignment_rows,
        pair_features,
        sequence_block_count,
        cluster_member_count,
        residue_present_mask,
        attention_in_weight,
        attention_out_weight,
        pair_bias_weight,
        outer_factor_weight,
        outer_output_weight,
        outer_product_bias,
    ):
        slots, rl, width = alignment_rows.shape
        heads = pair_bias_weight.shape[1]
        factor = outer_factor_weight.shape[1] // 2
        pair_width = outer_output_weight.shape[1]
        key_block = pair_features.shape[1]
        row_block = rl * n_res // n_seq
        tiles = rl // 2
        n_combos = 2 * n_res * tiles
        assert 2 * slots == LANES and tiles * factor == LANES and 4 * factor == LANES
        assert pair_width == LANES and heads == 8 and rl == 8
        assert key_block == 1 and rl % row_block == 0 and heads * rl < LANES
        any_space = pl.BlockSpec(memory_space=pltpu.HBM)
        vmem = pl.BlockSpec(memory_space=pltpu.VMEM)
        dma = pltpu.SemaphoreType.DMA
        operands = (
            sequence_block_count,
            residue_present_mask,
            alignment_rows,
            pair_features.reshape(rl, pair_features.shape[2]),
            cluster_member_count.reshape(1, slots),
            attention_in_weight,
            attention_out_weight,
            pair_bias_weight.T,
            outer_factor_weight,
            outer_output_weight,
            outer_product_bias.reshape(1, pair_width),
        )
        update, pair_update = pl.pallas_call(
            functools.partial(kernel, n_seq, n_res, slots, rl, heads, factor),
            out_shape=(
                pltpu.VMEM((slots, rl, width), BF16),
                pltpu.VMEM((row_block, rl, pair_width), BF16),
            ),
            in_specs=[any_space] * len(operands),
            out_specs=(vmem, vmem),
            scratch_shapes=[
                (pltpu.SMEM if at < 2 else pltpu.VMEM)(value.shape, value.dtype)
                for at, value in enumerate(operands)
            ]
            + [
                pltpu.VMEM((slots * rl, LANES), F32),
                pltpu.VMEM((tiles, width, LANES), F32),
                pltpu.VMEM((tiles, width, LANES), BF16),
                pltpu.VMEM((n_res - 1, tiles, width, LANES), BF16),
                pltpu.VMEM((1, LANES), F32),
                pltpu.VMEM((n_seq, 1, LANES), F32),
                pltpu.VMEM((tiles, 2 * LANES, 2 * LANES), BF16),
                pltpu.VMEM((4 * width, width), BF16),
                pltpu.VMEM((width, width), BF16),
                pltpu.VMEM((width, width), BF16),
                pltpu.VMEM((width, width), BF16),
                pltpu.VMEM((n_res, tiles, 2 * width, LANES), F32),
                pltpu.VMEM((n_res, tiles, 2 * width, LANES), F32),
                pltpu.VMEM((tiles, width, LANES), F32),
                pltpu.VMEM((tiles, n_combos, heads, LANES), F32),
                pltpu.VMEM((tiles, width, LANES), BF16),
                pltpu.VMEM((tiles, factor, LANES), BF16),
                pltpu.VMEM((n_res - 1, tiles, factor, LANES), BF16),
                pltpu.VMEM((2, factor * rl, LANES), F32),
                pltpu.VMEM((rl * rl, factor * factor), F32),
                pltpu.VMEM((factor * factor, pair_width), BF16),
                pltpu.VMEM((rl * n_res, rl, pair_width), BF16),
                pltpu.VMEM((n_seq - 1, row_block, rl, pair_width), BF16),
                dma((len(operands),)),
                dma((n_res - 1,)),
                dma((n_res - 1,)),
                dma((n_seq - 1,)),
                dma((n_seq - 1,)),
                dma((n_res - 1, tiles)),
                dma((n_res - 1, tiles)),
                dma((n_seq - 1,)),
                dma((n_seq - 1,)),
            ],
            compiler_params=pltpu.CompilerParams(collective_id=0, has_side_effects=True),
        )(*operands)
        return pl.pallas_call(
            finish,
            out_shape=(
                jax.ShapeDtypeStruct(update.shape, BF16),
                jax.ShapeDtypeStruct(pair_update.shape, BF16),
            ),
            in_specs=[vmem, vmem],
            out_specs=(any_space, any_space),
            scratch_shapes=[dma((2,))],
        )(
            pltpu.with_memory_space_constraint(update, pltpu.VMEM),
            pltpu.with_memory_space_constraint(pair_update, pltpu.VMEM),
        )

    return jax.shard_map(
        local,
        mesh=mesh,
        in_specs=(
            P("seq", "res", None),
            P("res", "seq", None),
            P("seq"),
            P("seq"),
            P(),
            P(),
            P(),
            P(),
            P(),
            P(),
            P(),
        ),
        out_specs=(P("seq", "res", None), P("seq", "res", None)),
        check_vma=False,
    )
```

```python
import functools
import math

import jax
import jax.numpy as jnp
from jax import lax
from jax.experimental import pallas as pl
from jax.experimental.pallas import tpu as pltpu
from jax.sharding import PartitionSpec as P

MESH = pl.DeviceIdType.MESH
F32 = jnp.float32
BF16 = jnp.bfloat16
LANES = 128


def dot(a, b, ca, cb, precision=None):
    return lax.dot_general(
        a, b, (((ca,), (cb,)), ((), ())), precision=precision, preferred_element_type=F32
    )


def norm_over(values, axis):
    centre = jnp.mean(values, axis=axis, keepdims=True)
    shifted = values - centre
    spread = jnp.mean(shifted * shifted, axis=axis, keepdims=True)
    return shifted * lax.rsqrt(spread + 1e-05)


def iota(shape, axis):
    return lax.broadcasted_iota(jnp.int32, shape, axis)


def ones_where(mask):
    return jnp.where(mask, 1.0, 0.0).astype(BF16)


def each(start, stop, body):
    if stop - start <= 16:
        for k in range(start, stop):
            body(k)
    else:
        pl.loop(start, stop)(body)


def drain(ref, sem):
    pltpu.make_async_copy(ref, ref, sem).wait()


def kernel(
    n_seq,
    n_res,
    slots,
    rl,
    heads,
    factor,
    count_hbm,
    mask_hbm,
    x_hbm,
    pair_hbm,
    members_hbm,
    w_in_hbm,
    w_out_hbm,
    w_bias_hbm,
    w_fac_hbm,
    w_proj_hbm,
    bias_hbm,
    update_ref,
    pair_out_ref,
    count_ref,
    mask_ref,
    x_ref,
    pair_ref,
    members_ref,
    w_in_ref,
    w_out_ref,
    w_bias_ref,
    w_fac_ref,
    w_raw,
    bias_ref,
    rows32,
    x_t,
    xn_buf,
    xn_recv,
    tile_buf,
    tile_recv,
    w_in_t,
    w_out_t,
    w_out_p,
    w_fac_t,
    kv_s,
    roll_s,
    gate_s,
    score_s,
    gated_s,
    left_buf,
    left_recv,
    right_s,
    w_perm,
    part_buf,
    part_recv,
    in_sem,
    xn_send_sem,
    xn_recv_sem,
    tile_send_sem,
    tile_recv_sem,
    left_send_sem,
    left_recv_sem,
    part_send_sem,
    part_recv_sem,
):
    me_s = lax.axis_index("seq")
    me_r = lax.axis_index("res")
    width = x_ref.shape[2]
    hd = width // heads
    tiles = rl // 2
    row_block = rl * n_res // n_seq

    def seq_peer(k):
        return lax.rem(me_s + k, n_seq)

    def res_peer(k):
        return lax.rem(me_r + k, n_res)

    def res_of(block):
        return lax.rem(me_r + n_res - block, n_res)

    barrier = pltpu.get_barrier_semaphore()

    def greet(k):
        pl.semaphore_signal(barrier, inc=1, device_id=(seq_peer(k), me_r), device_id_type=MESH)

    each(1, n_seq, greet)
    for k in range(1, n_res):
        pl.semaphore_signal(barrier, inc=1, device_id=(me_s, res_peer(k)), device_id_type=MESH)

    loads = {}
    for at, (name, src, dst) in enumerate(
        [
            ("pair", pair_hbm, pair_ref),
            ("w_bias", w_bias_hbm, w_bias_ref),
            ("count", count_hbm, count_ref),
            ("members", members_hbm, members_ref),
            ("x", x_hbm, x_ref),
            ("w_in", w_in_hbm, w_in_ref),
            ("mask", mask_hbm, mask_ref),
            ("w_out", w_out_hbm, w_out_ref),
            ("w_fac", w_fac_hbm, w_fac_ref),
            ("w_proj", w_proj_hbm, w_raw),
            ("bias", bias_hbm, bias_ref),
        ]
    ):
        loads[name] = pltpu.make_async_copy(src, dst, in_sem.at[at])
        loads[name].start()

    def loaded(*names):
        for name in names:
            loads[name].wait()

    lane = iota((1, LANES), 1)
    low = lane < slots
    of_head = iota((heads, LANES), 1) // rl == iota((heads, LANES), 0)

    loaded("pair", "w_bias", "count", "members")
    count = count_ref[0]
    usable = (lax.rem(lane, slots) < count).astype(F32)
    members = members_ref[...].astype(F32)
    members = jnp.concatenate([members, members], axis=1)
    seq_weight = members * usable
    own_weight = jnp.sum(jnp.where(low, seq_weight, 0.0), axis=1, keepdims=True)

    pair_norm = norm_over(pair_ref[...].astype(F32), 1)
    bias_t = dot(
        w_bias_ref[...],
        jnp.concatenate([pair_norm] * (LANES // rl), axis=0),
        1,
        1,
        lax.Precision.HIGHEST,
    )
    packed = jnp.sum(jnp.where(of_head, bias_t, 0.0), axis=0, keepdims=True)
    packed = jnp.where(lane == LANES - 1, own_weight, packed)
    tile_buf[...] = packed
    tile_recv[0] = packed

    loaded("x")
    rows32[:, :width] = x_ref[...].astype(F32).reshape(slots * rl, width)
    eye = ones_where(iota((width, width), 0) == iota((width, width), 1))
    all_rows = jnp.concatenate(
        [rows32[pl.ds(i, slots, stride=rl), :][:, :width] for i in range(rl)], axis=0
    ).astype(BF16)
    turned = dot(eye, all_rows, 1, 1)
    x_t[...] = turned
    x_norm = norm_over(turned, 0).astype(BF16)
    for t in range(tiles):
        xn_buf[t] = x_norm[:, t * LANES : (t + 1) * LANES]

    pl.semaphore_wait(barrier, n_seq - 1 + n_res - 1)

    def tile_send(k):
        pltpu.make_async_remote_copy(
            src_ref=tile_buf,
            dst_ref=tile_recv.at[k],
            send_sem=tile_send_sem,
            recv_sem=tile_recv_sem,
            device_id=(seq_peer(k), me_r),
            device_id_type=MESH,
        ).start()

    each(1, n_seq, tile_send)

    def xn_copy(k, t):
        return pltpu.make_async_remote_copy(
            src_ref=xn_buf.at[t],
            dst_ref=xn_recv.at[k - 1, t],
            send_sem=xn_send_sem,
            recv_sem=xn_recv_sem.at[k - 1, t],
            device_id=(me_s, res_peer(k)),
            device_id_type=MESH,
        )

    for k in range(1, n_res):
        for t in range(tiles):
            xn_copy(k, t).start()

    loaded("w_in", "mask", "w_out", "w_fac", "w_proj", "bias")
    groups_in = w_in_ref.shape[1]
    to_row, from_col = iota((groups_in, groups_in), 0), iota((groups_in, groups_in), 1)
    order = (
        to_row // width * width
        + lax.rem(to_row, heads) * hd
        + lax.rem(to_row, width) // heads
    )
    perm = ones_where(order == from_col)
    w_in_t[...] = dot(perm, w_in_ref[...], 1, 1).astype(BF16)
    perm_out = perm[:width, :width]
    w_out_t[...] = dot(w_out_ref[...], perm_out, 0, 1).astype(BF16)
    w_out_p[...] = dot(perm_out, w_out_ref[...], 1, 0).astype(BF16)
    w_fac_t[...] = dot(w_fac_ref[...], eye, 0, 0).astype(BF16)

    scale = 1.0 / math.sqrt(hd)

    def put_kv(block, t, kv):
        kv = kv.astype(BF16).astype(F32)
        kv_s[block, t] = kv
        roll_s[block, t] = pltpu.roll(kv, slots, 1)

    proj = dot(w_in_t[...], jnp.concatenate([xn_buf[t] for t in range(tiles)], axis=1), 1, 0)
    query = (proj[:width] * scale).astype(BF16).astype(F32)
    gate_s[...] = jax.nn.sigmoid(proj[3 * width :])
    queries = [query[:, t * LANES : (t + 1) * LANES] for t in range(tiles)]
    for t in range(tiles):
        put_kv(0, t, proj[width : 3 * width, t * LANES : (t + 1) * LANES])

    for d in range(factor):
        w_perm[d * factor : (d + 1) * factor] = w_raw[pl.ds(d, factor, stride=factor), :].astype(BF16)

    combos = [(turn, block, u) for turn in range(2) for block in range(n_res) for u in range(tiles)]

    def score(block, key_tile):
        for at, (turn, of, u) in enumerate(combos):
            if of != block or u != key_tile:
                continue
            source = (roll_s if turn else kv_s).at[block, u]
            for t in range(tiles):
                total = None
                for d in range(hd):
                    term = queries[t][d * heads : (d + 1) * heads] * source[d * heads : (d + 1) * heads]
                    total = term if total is None else total + term
                score_s[t, at] = total

    for u in range(tiles):
        score(0, u)
    for block in range(1, n_res):
        for u in range(tiles):
            xn_copy(block, u).wait_recv()
            put_kv(block, u, dot(w_in_t[width : 3 * width], xn_recv[block - 1, u], 1, 0))
            score(block, u)

    drain(tile_recv.at[pl.ds(1, n_seq - 1)], tile_recv_sem)

    weight_sum = jnp.sum(tile_recv[...], axis=0)[:, LANES - 1 : LANES]
    head_base = iota((heads, LANES), 0) * rl
    side = (iota((heads, LANES), 1) >= slots).astype(jnp.int32)
    picks = [head_base + 2 * t + side for t in range(tiles)]

    keyed = {}
    for block in range(n_res):
        for i in range(rl):
            j = res_of(block) * rl + i
            key_mask = jnp.where(mask_ref[j] == 1, 0.0, -1000000.0).astype(F32)
            row = tile_recv[lax.rem(me_s - j + n_seq, n_seq)] + key_mask
            keyed[block, i] = jnp.broadcast_to(row, (heads, LANES))

    for t in range(tiles):
        spread = {
            key: jnp.take_along_axis(row, picks[t], axis=1, mode="promise_in_bounds")
            for key, row in keyed.items()
        }
        scores = []
        for at, (turn, block, u) in enumerate(combos):
            near, far = spread[block, 2 * u + turn], spread[block, 2 * u + 1 - turn]
            scores.append(score_s[t, at] + jnp.where(low, near, far))
        top = functools.reduce(jnp.maximum, scores)
        context = [None] * hd
        mass = None
        for at, (turn, block, u) in enumerate(combos):
            source = (roll_s if turn else kv_s).at[block, u]
            expo = jnp.exp(scores[at] - top)
            mass = expo if mass is None else mass + expo
            for d in range(hd):
                term = expo * source[width + d * heads : width + (d + 1) * heads]
                context[d] = term if context[d] is None else context[d] + term
        norm = 1.0 / mass
        context = jnp.concatenate([c * norm for c in context], axis=0)
        gated_s[t] = (gate_s[:, t * LANES : (t + 1) * LANES] * context).astype(BF16)

    all_usable = jnp.concatenate([usable] * tiles, axis=1)
    keeps = [mask_ref[me_r * rl + i].astype(F32) for i in range(rl)]
    all_keep = jnp.concatenate(
        [jnp.where(low, keeps[2 * t], keeps[2 * t + 1]) for t in range(tiles)], axis=1
    )
    gated = jnp.concatenate([gated_s[t] for t in range(tiles)], axis=1)
    update = dot(w_out_t[...], gated, 1, 0).astype(BF16).astype(F32) * all_usable
    outer_norm = norm_over(x_t[...] + update, 0).astype(BF16)
    factors = dot(w_fac_t[...], outer_norm, 1, 0) * all_keep
    left = factors[:factor].astype(BF16)
    for t in range(tiles):
        left_buf[t] = left[:, t * LANES : (t + 1) * LANES]

    def left_copy(k):
        return pltpu.make_async_remote_copy(
            src_ref=left_buf,
            dst_ref=left_recv.at[k - 1],
            send_sem=left_send_sem,
            recv_sem=left_recv_sem.at[k - 1],
            device_id=(me_s, res_peer(k)),
            device_id_type=MESH,
        )

    for k in range(1, n_res):
        left_copy(k).start()

    for t in range(tiles):
        right = factors[factor:, t * LANES : (t + 1) * LANES] * seq_weight
        turned = pltpu.roll(right, slots, 1)
        right_s[0, pl.ds(2 * t, factor, stride=rl), :] = right
        right_s[0, pl.ds(2 * t + 1, factor, stride=rl), :] = turned
        right_s[1, pl.ds(2 * t, factor, stride=rl), :] = turned
        right_s[1, pl.ds(2 * t + 1, factor, stride=rl), :] = right

    groups = LANES // factor
    sides = []
    for pair in range(groups // 2):
        rows = []
        for g in range(factor // groups):
            at = (g * groups + 2 * pair) * rl
            rows.append(jnp.where(low, right_s[0, at : at + rl], right_s[1, at + rl : at + 2 * rl]))
        sides.append(jnp.concatenate(rows, axis=0))
    right_all = jnp.concatenate(sides, axis=1).astype(BF16)

    def project(block, left):
        blank = jnp.zeros((factor, LANES), BF16)
        outer = []
        for t in range(tiles):
            plain = left[t].astype(F32)
            turned = pltpu.roll(plain, slots, 1)
            spread = []
            for first, second in ((plain, turned), (turned, plain)):
                near = jnp.where(low, first, 0.0).astype(BF16)
                far = jnp.where(low, 0.0, second).astype(BF16)
                for pair in range(groups // 2):
                    for piece in (near, far):
                        cells = [blank] * (groups // 2)
                        cells[pair] = piece
                        spread.append(jnp.concatenate(cells, axis=1))
            spread = jnp.concatenate(spread, axis=0)
            products = dot(right_all, spread, 1, 1)
            for e in range(2):
                outer.append(
                    jnp.concatenate(
                        [
                            products[g * rl : (g + 1) * rl, e * LANES : (e + 1) * LANES]
                            for g in range(factor // groups)
                        ],
                        axis=1,
                    )
                )
        outer = jnp.concatenate(outer, axis=0).astype(BF16)
        part = dot(outer, w_perm[...], 1, 0)
        part_buf[pl.ds(res_of(block) * rl, rl)] = part.reshape(rl, rl, part.shape[1]).astype(BF16)

    def part_copy(owner, k):
        return pltpu.make_async_remote_copy(
            src_ref=part_buf.at[pl.ds(owner * row_block, row_block)],
            dst_ref=part_recv.at[k - 1],
            send_sem=part_send_sem,
            recv_sem=part_recv_sem,
            device_id=(owner, me_r),
            device_id_type=MESH,
        )

    def send_parts(block):
        for m in range(rl // row_block):
            owner = res_of(block) * (rl // row_block) + m
            offset = lax.rem(owner + n_seq - me_s, n_seq)

            @pl.when(offset > 0)
            def _():
                part_copy(owner, offset).start()

    project(0, left_buf[...])
    send_parts(0)
    for block in range(1, n_res):
        left_copy(block).wait_recv()
        project(block, left_recv[block - 1])
        send_parts(block)

    row_usable = (iota((slots, 1), 0) < count).astype(F32)
    w_out_wide = jnp.concatenate([w_out_p[...], w_out_p[...]], axis=1)
    for t in range(tiles):
        plain = dot(gated_s[t], w_out_wide, 0, 0).astype(BF16).astype(F32)
        for e in range(2):
            rows32[pl.ds(2 * t + e, slots, stride=rl), :] = (
                plain[e * slots : (e + 1) * slots] * row_usable
            )
    update_ref[...] = rows32[:, :width].reshape(slots, rl, width).astype(BF16)

    drain(tile_recv.at[pl.ds(1, n_seq - 1)], tile_send_sem)
    drain(xn_recv, xn_send_sem)
    drain(left_recv, left_send_sem)
    drain(part_recv, part_recv_sem)
    drain(part_recv, part_send_sem)

    own = part_buf[pl.ds(me_s * row_block, row_block)].astype(F32)
    total = own + jnp.sum(part_recv[...].astype(F32), axis=0)
    pair_out_ref[...] = (total / weight_sum[None] + bias_ref[...][None]).astype(BF16)


def finish(update_ref, pair_ref, update_hbm, pair_hbm, sem):
    copies = [
        pltpu.make_async_copy(update_ref, update_hbm, sem.at[0]),
        pltpu.make_async_copy(pair_ref, pair_hbm, sem.at[1]),
    ]
    for copy in copies:
        copy.start()
    for copy in copies:
        copy.wait()


def solution(mesh):
    n_seq = mesh.shape["seq"]
    n_res = mesh.shape["res"]

    def local(
        alignment_rows,
        pair_features,
        sequence_block_count,
        cluster_member_count,
        residue_present_mask,
        attention_in_weight,
        attention_out_weight,
        pair_bias_weight,
        outer_factor_weight,
        outer_output_weight,
        outer_product_bias,
    ):
        slots, rl, width = alignment_rows.shape
        heads = pair_bias_weight.shape[1]
        factor = outer_factor_weight.shape[1] // 2
        pair_width = outer_output_weight.shape[1]
        key_block = pair_features.shape[1]
        row_block = rl * n_res // n_seq
        tiles = rl // 2
        n_combos = 2 * n_res * tiles
        assert 2 * slots == LANES and tiles * factor == LANES and 4 * factor == LANES
        assert pair_width == LANES and heads == 8 and rl == 8
        assert key_block == 1 and rl % row_block == 0 and heads * rl < LANES
        any_space = pl.BlockSpec(memory_space=pltpu.HBM)
        vmem = pl.BlockSpec(memory_space=pltpu.VMEM)
        dma = pltpu.SemaphoreType.DMA
        operands = (
            sequence_block_count,
            residue_present_mask,
            alignment_rows,
            pair_features.reshape(rl, pair_features.shape[2]),
            cluster_member_count.reshape(1, slots),
            attention_in_weight,
            attention_out_weight,
            pair_bias_weight.T,
            outer_factor_weight,
            outer_output_weight,
            outer_product_bias.reshape(1, pair_width),
        )
        update, pair_update = pl.pallas_call(
            functools.partial(kernel, n_seq, n_res, slots, rl, heads, factor),
            out_shape=(
                pltpu.VMEM((slots, rl, width), BF16),
                pltpu.VMEM((row_block, rl, pair_width), BF16),
            ),
            in_specs=[any_space] * len(operands),
            out_specs=(vmem, vmem),
            scratch_shapes=[
                (pltpu.SMEM if at < 2 else pltpu.VMEM)(value.shape, value.dtype)
                for at, value in enumerate(operands)
            ]
            + [
                pltpu.VMEM((slots * rl, LANES), F32),
                pltpu.VMEM((width, tiles * LANES), F32),
                pltpu.VMEM((tiles, width, LANES), BF16),
                pltpu.VMEM((n_res - 1, tiles, width, LANES), BF16),
                pltpu.VMEM((1, LANES), F32),
                pltpu.VMEM((n_seq, 1, LANES), F32),
                pltpu.VMEM((4 * width, width), BF16),
                pltpu.VMEM((width, width), BF16),
                pltpu.VMEM((width, width), BF16),
                pltpu.VMEM((width, width), BF16),
                pltpu.VMEM((n_res, tiles, 2 * width, LANES), F32),
                pltpu.VMEM((n_res, tiles, 2 * width, LANES), F32),
                pltpu.VMEM((width, tiles * LANES), F32),
                pltpu.VMEM((tiles, n_combos, heads, LANES), F32),
                pltpu.VMEM((tiles, width, LANES), BF16),
                pltpu.VMEM((tiles, factor, LANES), BF16),
                pltpu.VMEM((n_res - 1, tiles, factor, LANES), BF16),
                pltpu.VMEM((2, factor * rl, LANES), F32),
                pltpu.VMEM((factor * factor, pair_width), BF16),
                pltpu.VMEM((rl * n_res, rl, pair_width), BF16),
                pltpu.VMEM((n_seq - 1, row_block, rl, pair_width), BF16),
                dma((len(operands),)),
                dma,
                dma((n_res - 1, tiles)),
                dma,
                dma,
                dma,
                dma((n_res - 1,)),
                dma,
                dma,
            ],
            compiler_params=pltpu.CompilerParams(collective_id=0, has_side_effects=True),
        )(*operands)
        return pl.pallas_call(
            finish,
            out_shape=(
                jax.ShapeDtypeStruct(update.shape, BF16),
                jax.ShapeDtypeStruct(pair_update.shape, BF16),
            ),
            in_specs=[vmem, vmem],
            out_specs=(any_space, any_space),
            scratch_shapes=[dma((2,))],
        )(
            pltpu.with_memory_space_constraint(update, pltpu.VMEM),
            pltpu.with_memory_space_constraint(pair_update, pltpu.VMEM),
        )

    return jax.shard_map(
        local,
        mesh=mesh,
        in_specs=(
            P("seq", "res", None),
            P("res", "seq", None),
            P("seq"),
            P("seq"),
            P(),
            P(),
            P(),
            P(),
            P(),
            P(),
            P(),
        ),
        out_specs=(P("seq", "res", None), P("seq", "res", None)),
        check_vma=False,
    )
```
